32 devices in a mesh: parts: 2 (over x), blk: 16 (over z, y, core).
Axes of the slice: x: 2, y: 2, z: 4, core: 2. Of those that a mesh axis runs over, the one named last changes fastest.
Arguments:
- embeddings: bfloat16 [8192, 1024], P(('parts', 'blk')), parts along dimension 0, may hold values from -6 to 6
- cluster: int32 [8192, 1], P(('parts', 'blk')), parts along dimension 0, may hold values from 0 to 15; in each aligned block of 256 rows (0 to 255, 256 to 511, ...) at most 32 rows name the same one
- rank: int32 [8192], P(('parts', 'blk')), parts along dimension 0, may hold values from 0 to 4095, each once
Outputs:
- best: float32 [8192], P(('parts', 'blk')), parts along dimension 0
The draws below stay inside these ranges and needn't reach their ends.
There are 2 independent parts, one for each index of `parts`. The reference program is written for one: setup_inputs(seed, part) draws one part's arguments, and reference() takes and returns one part's arrays. A program takes and returns all parts, laid end to end along the dimension named above; each array names one. Nothing has to cross between parts.
Inputs may be any that keep to these rules, and one draw needn't show every extreme that they name: Cluster c is kept by index c of blk. The rows of one device name one cluster at most 32 times, a bound that some block reaches. Each rank appears once in a group.
All inputs are finite; a program needn't handle non-finite values.
Results may differ from the reference program's by a relative error of at most 0.0013.
Values may be sent and summed in bfloat16 or wider, within the bound.
A program may use at most 64 MiB of HBM per device.

```python
import math
import jax
import jax.numpy as jnp
import numpy as np
from jax import lax

D = 1024
ROWS_DEV = 256
ROWS = 4096
CAP = 32
SLOTS = 512
N_BLK = 16


def levels(own_key, extent, split, least, top_value):
    level, own = 1.0, jax.random.fold_in(own_key, 6)
    for dim, parts in split:
        steps = jnp.exp(jax.random.uniform(jax.random.fold_in(own, dim), (parts,), jnp.float32, least / len(split), top_value / len(split)))
        level = level * jnp.repeat(steps, extent[dim] // parts).reshape([-1 if axis == dim else 1 for axis in range(len(extent))])
    return level


def assign_block(rng, own, number, rows, amount, top, most, skew):
    ranking = jax.random.permutation(rng, amount)
    heavy_load, ordinary = shares(amount, rows * top, most, skew, True), shares(amount, rows * top, most, skew, False)
    places = jnp.arange(amount)

    def named(tallies, turn):
        used = int((tallies > 0).sum())
        fixed = max(1, used // 4)
        moved = fixed + (places - fixed + turn * (used - fixed)) % max(1, amount - fixed)
        return jnp.zeros((amount,), jnp.int32).at[ranking[jnp.where(places < fixed, places, moved)]].set(jnp.asarray(tallies, jnp.int32))

    tallies = jnp.where(number % 4 == 0, named(heavy_load, number // 4), named(ordinary, number - number // 4 - 1))
    mixed = jax.random.permutation(jax.random.fold_in(own, 3), amount)
    donor, receiver = mixed[0:amount // 2 * 2:2], mixed[1:amount // 2 * 2:2]
    slack = jnp.minimum(tallies[donor] - 1, most - tallies[receiver]) // 2
    slack = jnp.where((donor == ranking[0]) | (receiver == ranking[0]) | (tallies[receiver] == 0), 0, jnp.maximum(slack, 0))
    moved = jax.random.randint(jax.random.fold_in(own, 4), (amount // 2,), 0, 1 << 20) % (slack + 1)
    tallies = tallies.at[donor].add(-moved).at[receiver].add(moved)
    items = jnp.searchsorted(jnp.cumsum(tallies), jnp.arange(rows * top), side="right").astype(jnp.int32)
    grid = items.reshape(top, rows).T
    grid = grid[jax.random.permutation(jax.random.fold_in(own, 1), rows)]
    turn = jax.random.randint(jax.random.fold_in(own, 2), (rows, 1), 0, top)
    return jnp.take_along_axis(grid, (jnp.arange(top)[None, :] + turn) % top, axis=1)


def shares(count, total, most, skew, full):
    loads = [(1 << 20) // math.isqrt(rank ** skew) + 1 for rank in range(1, count + 1)]
    largest = most if full else min(most, max(-(-total // count), total * loads[0] // sum(loads)))
    least = 1 if total - largest >= count - 1 else 0
    counts, surplus = [largest] + [least] * (count - 1), total - largest - least * (count - 1)
    while surplus > 0:
        candidates = [i for i in range(1, count) if counts[i] < largest] or [i for i in range(1, count) if counts[i] < most]
        pool, left = sum([loads[i] for i in candidates]), surplus
        for i in candidates:
            more = min(most - counts[i], max(1, left * loads[i] // pool), surplus)
            counts[i] = counts[i] + more
            surplus = surplus - more
    return np.array(counts)


def bell_draw(rng, extent, spread, reach, cuts=(), kind=jnp.bfloat16):
    loudness = levels(rng, extent, cuts, -0.22, 0.18) if cuts else 1.0
    drawn = jax.random.normal(rng, extent, jnp.float32) * spread * loudness
    return jnp.minimum(jnp.maximum(drawn, -reach), reach).astype(kind)


def setup_inputs(seed: int = 0, part: int = 0) -> dict:
    keys = jax.random.split(jax.random.key(seed), 4)
    own_keys = jax.random.split(jax.random.fold_in(keys[3], part), 4)
    embeddings = bell_draw(own_keys[0], (ROWS, D), 1.0, 6.0, ((0, 16),))
    cluster_keys = jax.random.split(jax.random.fold_in(own_keys[1], 1), ROWS // ROWS_DEV)
    cluster_turns = jax.random.permutation(jax.random.fold_in(own_keys[1], 3), ROWS // ROWS_DEV)
    cluster = jax.vmap(lambda own, number: assign_block(jax.random.fold_in(own_keys[1], 2), own, number, ROWS_DEV, N_BLK, 1, CAP, 2))(cluster_keys, cluster_turns).reshape((ROWS, 1))
    rank = jax.random.permutation(own_keys[2], ROWS).astype(jnp.int32)
    return {"embeddings": embeddings, "cluster": cluster, "rank": rank}


def reference(embeddings, cluster, rank):
    floats = embeddings.astype(jnp.float32)
    unit_rows = (floats * lax.rsqrt(lax.optimization_barrier(jnp.sum(floats * floats, axis=1, keepdims=True)) + 1e-06)).astype(jnp.bfloat16)
    labels = cluster[:, 0].astype(jnp.int32)
    grouping = jnp.argsort(labels, stable=True).astype(jnp.int32)
    grouped = unit_rows[grouping]
    group_rank = rank[grouping].astype(jnp.int32)
    group_ids = labels[grouping]
    counted = lax.optimization_barrier(jnp.sum((labels[:, None] == jnp.arange(N_BLK, dtype=jnp.int32)[None, :]).astype(jnp.int32), axis=0))
    starts = (jnp.cumsum(counted) - counted).astype(jnp.int32)
    padded_rows = jnp.concatenate([grouped, jnp.zeros((SLOTS, grouped.shape[1]), jnp.bfloat16)], axis=0)
    padded_rank = jnp.concatenate([group_rank, jnp.full((SLOTS,), -1, jnp.int32)], axis=0)
    padded_ids = jnp.concatenate([group_ids, jnp.full((SLOTS,), -1, jnp.int32)], axis=0)

    def one_cluster(which):
        begin_at = starts[which]
        window = lax.dynamic_slice_in_dim(padded_rows, begin_at, SLOTS, 0)
        win_rank = lax.dynamic_slice_in_dim(padded_rank, begin_at, SLOTS, 0)
        win_ids = lax.dynamic_slice_in_dim(padded_ids, begin_at, SLOTS, 0)
        similar = jnp.dot(window, window.T, preferred_element_type=jnp.float32)
        allowed = (win_ids[None, :] == which) & (win_rank[None, :] > win_rank[:, None])
        return lax.optimization_barrier(jnp.max(jnp.where(allowed, similar, -1.0), axis=1))
    results = lax.map(one_cluster, jnp.arange(N_BLK, dtype=jnp.int32))
    offsets = jnp.arange(ROWS, dtype=jnp.int32) - starts[group_ids]
    group_best = results[group_ids, offsets]
    return jnp.zeros((ROWS,), jnp.float32).at[grouping].set(group_best)
```

```python
import functools

import jax
import jax.numpy as jnp
from jax import lax
from jax.experimental import pallas as pl
from jax.experimental.pallas import tpu as pltpu
from jax.sharding import PartitionSpec as P

MESH = pl.DeviceIdType.MESH
HIGHEST = lax.Precision.HIGHEST


def best_over(q_rows, q_rank, k_rows, k_rank):
    total = q_rows.shape[0]
    block_len = min(512, total)
    similar = lax.dot_general(
        q_rows, k_rows, (((1,), (1,)), ((), ())), preferred_element_type=jnp.float32
    )
    allowed = k_rank[None, :] > q_rank[0:block_len, None]
    pieces = jnp.max(jnp.where(allowed, similar, -1.0), axis=1)
    return pieces


def local(embeddings, cluster, rank):
    devices = lax.axis_size("blk")
    local_rows = embeddings.shape[0]
    width = embeddings.shape[1]
    slot_total = 2 * local_rows
    capacity = slot_total // devices
    floats = embeddings.astype(jnp.float32)
    unit_rows = (
        floats * lax.rsqrt(jnp.sum(floats * floats, axis=1, keepdims=True) + 1e-06)
    ).astype(jnp.bfloat16)
    target = cluster[:, 0]
    one_hot = (target[:, None] == jnp.arange(devices, dtype=jnp.int32)[None, :]).astype(jnp.int32)
    earlier = jnp.cumsum(one_hot, axis=0) - one_hot
    within = jnp.sum(earlier * one_hot, axis=1)
    slot_of = target * capacity + within
    send_rows = (
        jnp.zeros((slot_total, width), jnp.bfloat16)
        .at[slot_of]
        .set(unit_rows)
        .reshape(devices, capacity, width)
    )
    send_rank = (
        jnp.full((slot_total,), -1, jnp.int32).at[slot_of].set(rank).reshape(devices, capacity)
    )
    got_rows, got_rank = (
        lax.all_to_all(send_rows, "blk", split_axis=0, concat_axis=0, tiled=True),
        lax.all_to_all(send_rank, "blk", split_axis=0, concat_axis=0, tiled=True),
    )
    all_rows = got_rows.reshape(slot_total, width)
    all_rank = got_rank.reshape(slot_total)
    best_flat = best_over(all_rows, all_rank, all_rows, all_rank)
    returned = lax.all_to_all(
        best_flat.reshape(devices, capacity), "blk", split_axis=0, concat_axis=0, tiled=True
    )
    return returned.reshape(slot_total)[slot_of]


def kernel(
    n, cap, emb_hbm, cluster_hbm, rank_hbm, out_ref,
    emb, cluster_ref, rank_ref, send_rows, rows, send_rank, ranks, send_best, bests,
    load_sems, row_out, row_in, rank_out, rank_in, best_out, best_in, edge_in, half_in, all_in,
):
    me = lax.axis_index("blk")
    count, width = emb.shape
    slots = n * cap
    quarter = n // 4
    part = quarter * cap
    early = quarter // 2
    layer = me // quarter
    turn = me % quarter
    side = layer // 2
    middle = jnp.logical_or(layer == 1, layer == 2)
    near = 1 + layer % 2
    rim = 3 * side
    far_rim = 3 - rim
    last = 2 - side
    inward = near * quarter
    across = last * quarter
    own = me - turn

    barrier = pltpu.get_barrier_semaphore()
    loads = [
        pltpu.make_async_copy(source, into, load_sems.at[i])
        for i, (source, into) in enumerate(
            [(cluster_hbm, cluster_ref), (rank_hbm, rank_ref), (emb_hbm, emb)]
        )
    ]

    def signal(sem, to):
        pl.semaphore_signal(sem, inc=1, device_id={"blk": to}, device_id_type=MESH)

    @pl.when(middle)
    def _():
        @pl.loop(0, quarter)
        def _(k):
            signal(barrier, inward + k)

        @pl.loop(0, quarter)
        def _(k):
            signal(barrier, rim * quarter + k)

        @pl.loop(1, quarter)
        def _(k):
            signal(barrier, own + lax.rem(turn + k, quarter))

    for load in loads:
        load.start()

    loads[0].wait()
    target = cluster_ref[...]
    ids = lax.broadcasted_iota(jnp.int32, (n, count), 0)
    named = (ids == target).astype(jnp.float32)
    before = lax.broadcasted_iota(jnp.int32, (count, count), 0)
    after = lax.broadcasted_iota(jnp.int32, (count, count), 1)
    upper = (before < after).astype(jnp.bfloat16)
    earlier = jnp.dot(named.astype(jnp.bfloat16), upper, preferred_element_type=jnp.float32)
    within = jnp.sum(earlier * named, axis=0, keepdims=True).astype(jnp.int32)
    slot_of = target * cap + within
    loads[2].wait()

    def pack(to):
        wanted = lax.broadcasted_iota(jnp.int32, (cap, count), 0) + to * cap
        pick = (wanted == slot_of).astype(jnp.bfloat16)
        floats = jnp.dot(pick, emb[...], preferred_element_type=jnp.float32)
        scale = lax.rsqrt(jnp.sum(floats * floats, axis=1, keepdims=True) + 1e-06)
        send_rows[to] = (floats * scale).astype(jnp.bfloat16)

    def row_copy(to):
        return pltpu.make_async_remote_copy(
            src_ref=send_rows.at[to], dst_ref=rows.at[me], send_sem=row_out.at[to],
            recv_sem=row_in.at[me], device_id={"blk": to}, device_id_type=MESH,
        )

    def row_arrival(source):
        return pltpu.make_async_remote_copy(
            src_ref=send_rows.at[source], dst_ref=rows.at[source], send_sem=row_out.at[source],
            recv_sem=row_in.at[source], device_id={"blk": source}, device_id_type=MESH,
        )

    def rank_copy(to, at):
        return pltpu.make_async_remote_copy(
            src_ref=send_rank.at[to], dst_ref=ranks.at[at], send_sem=rank_out.at[to],
            recv_sem=rank_in.at[at], device_id={"blk": to}, device_id_type=MESH,
        )

    per = 128 // cap

    def best_copy(to, at):
        return pltpu.make_async_remote_copy(
            src_ref=send_best.at[to // per], dst_ref=bests.at[at], send_sem=best_out.at[to],
            recv_sem=best_in.at[at], device_id={"blk": to}, device_id_type=MESH,
        )

    def turned(k):
        return lax.rem(turn + k, quarter)

    def pack_all(first, begin, end):
        @pl.loop(begin, end)
        def _(k):
            pack(first + turned(k))

    def send_all(first, begin, end):
        @pl.loop(begin, end)
        def _(k):
            row_copy(first + turned(k)).start()

    def pack_send(first, begin, end):
        @pl.loop(begin, end)
        def _(k):
            to = first + turned(k)
            pack(to)
            row_copy(to).start()

    pack(inward + turn)

    @pl.when(middle)
    def _():
        pl.semaphore_wait(barrier, 2 * quarter - 1)

    @pl.when(jnp.logical_not(middle))
    def _():
        pl.semaphore_wait(barrier, quarter)

        @pl.loop(0, quarter)
        def _(k):
            signal(edge_in, inward + k)

    row_copy(inward + turn).start()
    pack_send(inward, 1, early)
    loads[1].wait()
    lanes = lax.broadcasted_iota(jnp.int32, (128, count), 0)
    spots = (lanes == within).astype(jnp.float32)
    placed = lax.dot_general(
        named * (rank_ref[...] + 1).astype(jnp.float32), spots, (((1,), (1,)), ((), ())),
        precision=HIGHEST, preferred_element_type=jnp.float32,
    )
    for c in range(n):
        send_rank[c] = placed[c:c + 1]

    def rank_all(first, begin):
        @pl.loop(begin, quarter)
        def _(k):
            rank_copy(first + turned(k), me).start()

    rank_all(inward, 0)

    @pl.when(middle)
    def _():
        rank_all(own, 1)
        pack_send(own, 1, quarter)
        pl.semaphore_wait(edge_in, quarter)
        signal(half_in, inward + turn)
        rank_all(rim * quarter, 0)
        pack_all(far_rim * quarter, 0, quarter)
        pl.semaphore_wait(half_in, 1)
        signal(all_in, rim * quarter + turn)
        rank_all(far_rim * quarter, 0)
        send_all(far_rim * quarter, 0, quarter)
        pack_send(rim * quarter, 0, quarter)
        pack_send(inward, early, quarter)

    @pl.when(jnp.logical_not(middle))
    def _():
        pack_send(inward, early, quarter)
        pack_all(far_rim * quarter, 0, quarter)
        pack_all(own, 1, quarter)
        pl.semaphore_wait(all_in, 1)
        rank_all(own, 1)
        rank_all(far_rim * quarter, 0)
        rank_all(across, 0)
        send_all(far_rim * quarter, 0, quarter)
        send_all(own, 1, quarter)
        pack_send(across, 0, quarter)

    pack(me)
    rows[me] = send_rows[me]
    ranks[me] = send_rank[me]

    @pl.loop(1, n)
    def _(k):
        at = lax.rem(me + k, n)
        rank_copy(at, at).wait()

    order = [0, 1 + side, 3, last]
    held = jnp.concatenate(
        [ranks[g * quarter + k] for g in order for k in range(quarter)], axis=0
    )
    source = lax.broadcasted_iota(jnp.int32, (n, slots), 0)
    slot = lax.broadcasted_iota(jnp.int32, (n, slots), 1)
    spread = (slot // cap == source).astype(jnp.float32)
    wide = lax.dot_general(
        held, spread, (((0,), (0,)), ((), ())),
        precision=HIGHEST, preferred_element_type=jnp.float32,
    )
    lane_of = lax.broadcasted_iota(jnp.int32, (128, slots), 0)
    slot_in = lax.broadcasted_iota(jnp.int32, (128, slots), 1) % cap
    rank_row = jnp.sum(jnp.where(lane_of == slot_in, wide, 0.0), axis=0, keepdims=True)
    down = lax.dot_general(
        spread, held, (((0,), (0,)), ((), ())),
        precision=HIGHEST, preferred_element_type=jnp.float32,
    )
    lane_at = lax.broadcasted_iota(jnp.int32, (slots, 128), 1)
    slot_at = lax.broadcasted_iota(jnp.int32, (slots, 128), 0) % cap
    rank_col = jnp.sum(jnp.where(lane_at == slot_at, down, 0.0), axis=1, keepdims=True)

    @pl.loop(0, n)
    def _(k):
        @pl.when(jnp.logical_and(k != me, k // quarter != last))
        def _():
            row_arrival(k).wait_recv()

    def group(g):
        return rows[pl.ds(g * quarter, quarter)].reshape(part, width)

    def best_of(keys, key_rank, queries, query_rank):
        similar = lax.dot_general(
            keys, queries, (((1,), (1,)), ((), ())), preferred_element_type=jnp.float32
        )
        return jnp.max(jnp.where(key_rank > query_rank, similar, -1.0), axis=0, keepdims=True)

    head = 3 * part
    first = jnp.concatenate([group(g) for g in order[:3]], axis=0)
    best_first = best_of(first, rank_col[:head], first, rank_row[:, :head])

    @pl.loop(0, quarter)
    def _(k):
        row_arrival(across + k).wait_recv()

    tail = group(last)
    best_first = jnp.maximum(
        best_first, best_of(tail, rank_col[head:], first, rank_row[:, :head])
    )
    best_tail = jnp.maximum(
        best_of(first, rank_col[:head], tail, rank_row[:, head:]),
        best_of(tail, rank_col[head:], tail, rank_row[:, head:]),
    )
    for i, g in enumerate(order[:3]):
        send_best[g] = best_first[:, part * i:part * (i + 1)]
    send_best[last] = best_tail

    @pl.loop(0, n)
    def _(to):
        @pl.when(to != me)
        def _():
            best_copy(to, me).start()

    bests[me] = send_best[me // per]

    @pl.loop(0, n)
    def _(to):
        @pl.when(to != me)
        def _():
            row_copy(to).wait_send()

    @pl.loop(1, n)
    def _(k):
        at = lax.rem(me + k, n)
        best_copy(at, at).wait()

    mine = jnp.concatenate([bests[c] for c in range(n)], axis=0)
    place = (me % per) * cap + within
    for k in range(count // 128):
        piece = slice(128 * k, 128 * (k + 1))
        at = jnp.broadcast_to(place[:, piece], (n, 128))
        found = jnp.take_along_axis(mine, at, axis=1, mode="promise_in_bounds")
        out_ref[:, piece] = jnp.sum(
            jnp.where(named[:, piece] > 0.0, found, 0.0), axis=0, keepdims=True
        )


def fused(embeddings, cluster, rank):
    n = lax.axis_size("blk")
    count, width = embeddings.shape
    cap = 2 * count // n
    slots = n * cap
    vmem = pl.BlockSpec(memory_space=pltpu.VMEM)
    best = pl.pallas_call(
        functools.partial(kernel, n, cap),
        out_shape=pltpu.VMEM((1, count), jnp.float32),
        in_specs=[pl.BlockSpec(memory_space=pl.ANY)] * 3,
        out_specs=vmem,
        scratch_shapes=[
            pltpu.VMEM((count, width), jnp.bfloat16),
            pltpu.VMEM((1, count), jnp.int32),
            pltpu.VMEM((1, count), jnp.int32),
            pltpu.VMEM((n, cap, width), jnp.bfloat16),
            pltpu.VMEM((n, cap, width), jnp.bfloat16),
            pltpu.VMEM((n, 1, 128), jnp.float32),
            pltpu.VMEM((n, 1, 128), jnp.float32),
            pltpu.VMEM((slots // 128, 1, 128), jnp.float32),
            pltpu.VMEM((n, 1, 128), jnp.float32),
            pltpu.SemaphoreType.DMA((3,)),
        ] + [pltpu.SemaphoreType.DMA((n,))] * 6 + [pltpu.SemaphoreType.REGULAR] * 3,
        compiler_params=pltpu.CompilerParams(collective_id=0, has_side_effects=True),
    )(embeddings, cluster.reshape(1, count), rank.reshape(1, count))
    return best.reshape(count)


def solution(mesh):
    def body(embeddings, cluster, rank):
        n = lax.axis_size("blk")
        slots = 2 * embeddings.shape[0]
        cap = slots // n
        if n % 4 == 0 and slots == 512 and n // 4 * cap == 128:
            return fused(embeddings, cluster, rank)
        return local(embeddings, cluster, rank)

    return jax.shard_map(
        body,
        mesh=mesh,
        in_specs=(P(("parts", "blk"), None), P(("parts", "blk"), None), P(("parts", "blk"))),
        out_specs=P(("parts", "blk")),
        check_vma=False,
    )
```

```python
import functools

import jax
import jax.numpy as jnp
from jax import lax
from jax.experimental import pallas as pl
from jax.experimental.pallas import tpu as pltpu
from jax.sharding import PartitionSpec as P

MESH = pl.DeviceIdType.MESH
HIGHEST = lax.Precision.HIGHEST


def best_over(q_rows, q_rank, k_rows, k_rank):
    total = q_rows.shape[0]
    block_len = min(512, total)
    similar = lax.dot_general(
        q_rows, k_rows, (((1,), (1,)), ((), ())), preferred_element_type=jnp.float32
    )
    allowed = k_rank[None, :] > q_rank[0:block_len, None]
    pieces = jnp.max(jnp.where(allowed, similar, -1.0), axis=1)
    return pieces


def local(embeddings, cluster, rank):
    devices = lax.axis_size("blk")
    local_rows = embeddings.shape[0]
    width = embeddings.shape[1]
    slot_total = 2 * local_rows
    capacity = slot_total // devices
    floats = embeddings.astype(jnp.float32)
    unit_rows = (
        floats * lax.rsqrt(jnp.sum(floats * floats, axis=1, keepdims=True) + 1e-06)
    ).astype(jnp.bfloat16)
    target = cluster[:, 0]
    one_hot = (target[:, None] == jnp.arange(devices, dtype=jnp.int32)[None, :]).astype(jnp.int32)
    earlier = jnp.cumsum(one_hot, axis=0) - one_hot
    within = jnp.sum(earlier * one_hot, axis=1)
    slot_of = target * capacity + within
    send_rows = (
        jnp.zeros((slot_total, width), jnp.bfloat16)
        .at[slot_of]
        .set(unit_rows)
        .reshape(devices, capacity, width)
    )
    send_rank = (
        jnp.full((slot_total,), -1, jnp.int32).at[slot_of].set(rank).reshape(devices, capacity)
    )
    got_rows, got_rank = (
        lax.all_to_all(send_rows, "blk", split_axis=0, concat_axis=0, tiled=True),
        lax.all_to_all(send_rank, "blk", split_axis=0, concat_axis=0, tiled=True),
    )
    all_rows = got_rows.reshape(slot_total, width)
    all_rank = got_rank.reshape(slot_total)
    best_flat = best_over(all_rows, all_rank, all_rows, all_rank)
    returned = lax.all_to_all(
        best_flat.reshape(devices, capacity), "blk", split_axis=0, concat_axis=0, tiled=True
    )
    return returned.reshape(slot_total)[slot_of]


def kernel(
    n, cap, emb_hbm, cluster_hbm, rank_hbm, out_ref,
    emb, cluster_ref, rank_ref, send_rows, rows, send_rank, ranks, send_best, bests,
    load_sems, row_out, row_in, rank_out, rank_in, best_out, best_in, edge_in, half_in, all_in,
):
    me = lax.axis_index("blk")
    count, width = emb.shape
    slots = n * cap
    quarter = n // 4
    part = quarter * cap
    layer = me // quarter
    turn = me % quarter
    side = layer // 2
    early = quarter - 1
    middle = jnp.logical_or(layer == 1, layer == 2)
    near = 1 + layer % 2
    rim = 3 * side
    far_rim = 3 - rim
    last = 2 - side
    inward = near * quarter
    across = last * quarter
    own = me - turn

    barrier = pltpu.get_barrier_semaphore()
    loads = [
        pltpu.make_async_copy(source, into, load_sems.at[i])
        for i, (source, into) in enumerate(
            [(cluster_hbm, cluster_ref), (rank_hbm, rank_ref), (emb_hbm, emb)]
        )
    ]

    for load in loads:
        load.start()

    def signal(sem, to):
        pl.semaphore_signal(sem, inc=1, device_id={"blk": to}, device_id_type=MESH)

    @pl.when(middle)
    def _():
        @pl.loop(0, quarter)
        def _(k):
            signal(barrier, inward + k)

        @pl.loop(0, quarter)
        def _(k):
            signal(barrier, rim * quarter + k)

        @pl.loop(1, quarter)
        def _(k):
            signal(barrier, own + lax.rem(turn + k, quarter))

    loads[0].wait()
    target = cluster_ref[...]
    ids = lax.broadcasted_iota(jnp.int32, (n, count), 0)
    named = (ids == target).astype(jnp.float32)
    before = lax.broadcasted_iota(jnp.int32, (count, count), 0)
    after = lax.broadcasted_iota(jnp.int32, (count, count), 1)
    upper = (before < after).astype(jnp.bfloat16)
    earlier = jnp.dot(named.astype(jnp.bfloat16), upper, preferred_element_type=jnp.float32)
    within = jnp.sum(earlier * named, axis=0, keepdims=True).astype(jnp.int32)
    slot_of = target * cap + within
    def choose(to):
        wanted = lax.broadcasted_iota(jnp.int32, (cap, count), 0) + to * cap
        return (wanted == slot_of).astype(jnp.bfloat16)

    def pack(to, pick=None):
        pick = choose(to) if pick is None else pick
        floats = jnp.dot(pick, emb[...], preferred_element_type=jnp.float32)
        scale = lax.rsqrt(jnp.sum(floats * floats, axis=1, keepdims=True) + 1e-06)
        send_rows[to] = (floats * scale).astype(jnp.bfloat16)

    def place_of(source, keeper):
        z = source // quarter
        end = 2 - keeper // (2 * quarter)
        step = source % quarter
        wait = lax.rem(step - keeper % quarter + 2 + quarter, quarter)
        return jnp.where(z == end, 3 * quarter + wait, (z + 1) // 2 * quarter + step)

    def row_copy(to, at=None):
        at = place_of(me, to) if at is None else at
        return pltpu.make_async_remote_copy(
            src_ref=send_rows.at[to], dst_ref=rows.at[at], send_sem=row_out.at[to],
            recv_sem=row_in.at[at], device_id={"blk": to}, device_id_type=MESH,
        )

    def rank_copy(to, at=None):
        at = place_of(me, to) if at is None else at
        return pltpu.make_async_remote_copy(
            src_ref=send_rank.at[to], dst_ref=ranks.at[at], send_sem=rank_out.at[to],
            recv_sem=rank_in.at[at], device_id={"blk": to}, device_id_type=MESH,
        )

    other = lax.rem(me + 1, n)
    home = place_of(me, me)

    per = 128 // cap

    def best_copy(to, at):
        return pltpu.make_async_remote_copy(
            src_ref=send_best.at[place_of(to, me) // per], dst_ref=bests.at[at], send_sem=best_out.at[to],
            recv_sem=best_in.at[at], device_id={"blk": to}, device_id_type=MESH,
        )

    def turned(k):
        odd = turn % 2
        cross = (1 - odd) * lax.rem(k + 1, 2) + odd * lax.rem((k + 1) // 2, 2)
        return lax.rem(turn // 2 + cross, 2) * 2 + lax.rem(turn + k // 2, 2)

    def pack_all(first, begin, end):
        @pl.loop(begin, end)
        def _(k):
            pack(first + turned(k))

    def send_all(first, begin, end):
        @pl.loop(begin, end)
        def _(k):
            row_copy(first + turned(k)).start()

    def pack_send(first, begin, end):
        @pl.loop(begin, end)
        def _(k):
            to = first + turned(k)
            pack(to)
            row_copy(to).start()

    lead = inward + turned(0)
    pick_lead = choose(lead)
    loads[2].wait()
    pack(lead, pick_lead)

    @pl.when(middle)
    def _():
        pl.semaphore_wait(barrier, 2 * quarter - 1)

    @pl.when(jnp.logical_not(middle))
    def _():
        pl.semaphore_wait(barrier, quarter)

        @pl.loop(0, quarter)
        def _(k):
            signal(edge_in, inward + k)

    row_copy(lead).start()
    pack_send(inward, 1, 2)
    loads[1].wait()
    lanes = lax.broadcasted_iota(jnp.int32, (128, count), 0)
    spots = (lanes == within).astype(jnp.float32)
    placed = lax.dot_general(
        named * (rank_ref[...] + 1).astype(jnp.float32), spots, (((1,), (1,)), ((), ())),
        precision=HIGHEST, preferred_element_type=jnp.float32,
    )
    for c in range(n):
        send_rank[c] = placed[c:c + 1]

    def rank_all(first, begin):
        @pl.loop(begin, quarter)
        def _(k):
            rank_copy(first + lax.rem(turn + k, quarter)).start()

    def send_own():
        @pl.loop(1, quarter)
        def _(k):
            to = own + lax.rem(turn + k, quarter)
            pack(to)
            row_copy(to).start()

    rank_all(inward, 0)

    @pl.when(middle)
    def _():
        pl.semaphore_wait(edge_in, quarter)
        signal(half_in, inward + turn)
        pack_send(inward, 2, early)
        rank_all(rim * quarter, 0)
        rank_all(own, 1)
        pack_send(rim * quarter, 0, quarter)
        pl.semaphore_wait(half_in, 1)
        signal(all_in, rim * quarter + turn)
        rank_all(far_rim * quarter, 0)
        pack_send(far_rim * quarter, 0, quarter)
        pack_send(inward, early, quarter)
        send_own()

    @pl.when(jnp.logical_not(middle))
    def _():
        pack_send(inward, 2, quarter)
        pack_all(far_rim * quarter, 0, quarter)
        pl.semaphore_wait(all_in, 1)
        rank_all(far_rim * quarter, 0)
        rank_all(across, 0)
        rank_all(own, 1)
        send_all(far_rim * quarter, 0, quarter)
        pack_send(across, 0, quarter)
        send_own()

    pack(me)
    rows[home] = send_rows[me]
    ranks[home] = send_rank[me]

    @pl.loop(1, n)
    def _(k):
        rank_copy(lax.rem(me + k, n)).wait_send()

    @pl.loop(0, n)
    def _(k):
        @pl.when(k != home)
        def _():
            rank_copy(other, k).wait_recv()

    held = jnp.concatenate([ranks[c] for c in range(n)], axis=0)
    source = lax.broadcasted_iota(jnp.int32, (n, slots), 0)
    slot = lax.broadcasted_iota(jnp.int32, (n, slots), 1)
    spread = (slot // cap == source).astype(jnp.float32)
    wide = lax.dot_general(
        held, spread, (((0,), (0,)), ((), ())),
        precision=HIGHEST, preferred_element_type=jnp.float32,
    )
    lane_of = lax.broadcasted_iota(jnp.int32, (128, slots), 0)
    slot_in = lax.broadcasted_iota(jnp.int32, (128, slots), 1) % cap
    rank_row = jnp.sum(jnp.where(lane_of == slot_in, wide, 0.0), axis=0, keepdims=True)
    down = lax.dot_general(
        spread, held, (((0,), (0,)), ((), ())),
        precision=HIGHEST, preferred_element_type=jnp.float32,
    )
    lane_at = lax.broadcasted_iota(jnp.int32, (slots, 128), 1)
    slot_at = lax.broadcasted_iota(jnp.int32, (slots, 128), 0) % cap
    rank_col = jnp.sum(jnp.where(lane_at == slot_at, down, 0.0), axis=1, keepdims=True)

    def best_of(keys, key_rank, queries, query_rank):
        similar = lax.dot_general(
            keys, queries, (((1,), (1,)), ((), ())), preferred_element_type=jnp.float32
        )
        return jnp.max(jnp.where(key_rank > query_rank, similar, -1.0), axis=0, keepdims=True)

    def arrive(begin, end):
        @pl.loop(begin, end)
        def _(k):
            @pl.when(k != home)
            def _():
                row_copy(other, k).wait_recv()

    def send_back(begin, end):
        @pl.loop(begin, end)
        def _(to):
            @pl.when(to != me)
            def _():
                best_copy(to, me).start()

    def span(begin, end):
        return rows[begin:end].reshape((end - begin) * cap, width)

    early_row, late_row = rank_row[:, :3 * part], rank_row[:, 3 * part:]
    early_col, late_col = rank_col[:3 * part], rank_col[3 * part:]
    arrive(0, n - quarter)
    best_early = best_of(span(0, n - quarter), early_col, span(0, n - quarter), early_row)
    arrive(n - quarter, n)
    fresh = span(n - quarter, n)
    send_best[0] = jnp.maximum(
        best_early[:, :part], best_of(fresh, late_col, span(0, quarter), early_row[:, :part])
    )
    send_back(0, quarter)
    best_rest = jnp.maximum(
        best_early[:, part:],
        best_of(fresh, late_col, span(quarter, n - quarter), early_row[:, part:]),
    )
    best_late = jnp.maximum(
        best_of(span(0, n - quarter), early_col, fresh, late_row),
        best_of(fresh, late_col, fresh, late_row),
    )
    send_best[1] = best_rest[:, :part]
    send_best[2] = best_rest[:, part:]
    send_best[3] = best_late
    send_back(quarter, n)
    bests[me] = send_best[home // per]

    keeper = lax.broadcasted_iota(jnp.int32, (n, 128), 0)
    offset = jnp.zeros((n, 128), jnp.int32)
    for c in range(n):
        offset = jnp.where(keeper == c, place_of(me, c) % per * cap, offset)

    @pl.loop(0, n)
    def _(to):
        @pl.when(to != me)
        def _():
            row_copy(to).wait_send()

    @pl.loop(1, n)
    def _(k):
        at = lax.rem(me + k, n)
        best_copy(at, at).wait()

    mine = jnp.concatenate([bests[c] for c in range(n)], axis=0)
    for k in range(count // 128):
        piece = slice(128 * k, 128 * (k + 1))
        at = offset + within[:, piece]
        found = jnp.take_along_axis(mine, at, axis=1, mode="promise_in_bounds")
        out_ref[:, piece] = jnp.sum(
            jnp.where(named[:, piece] > 0.0, found, 0.0), axis=0, keepdims=True
        )


def fused(embeddings, cluster, rank):
    n = lax.axis_size("blk")
    count, width = embeddings.shape
    cap = 2 * count // n
    slots = n * cap
    vmem = pl.BlockSpec(memory_space=pltpu.VMEM)
    best = pl.pallas_call(
        functools.partial(kernel, n, cap),
        out_shape=pltpu.VMEM((1, count), jnp.float32),
        in_specs=[pl.BlockSpec(memory_space=pl.ANY)] * 3,
        out_specs=vmem,
        scratch_shapes=[
            pltpu.VMEM((count, width), jnp.bfloat16),
            pltpu.VMEM((1, count), jnp.int32),
            pltpu.VMEM((1, count), jnp.int32),
            pltpu.VMEM((n, cap, width), jnp.bfloat16),
            pltpu.VMEM((n, cap, width), jnp.bfloat16),
            pltpu.VMEM((n, 1, 128), jnp.float32),
            pltpu.VMEM((n, 1, 128), jnp.float32),
            pltpu.VMEM((slots // 128, 1, 128), jnp.float32),
            pltpu.VMEM((n, 1, 128), jnp.float32),
            pltpu.SemaphoreType.DMA((3,)),
        ] + [pltpu.SemaphoreType.DMA((n,))] * 6 + [pltpu.SemaphoreType.REGULAR] * 3,
        compiler_params=pltpu.CompilerParams(collective_id=0, has_side_effects=True),
    )(embeddings, cluster.reshape(1, count), rank.reshape(1, count))
    return best.reshape(count)


def solution(mesh):
    def body(embeddings, cluster, rank):
        n = lax.axis_size("blk")
        slots = 2 * embeddings.shape[0]
        cap = slots // n
        if n == 16 and slots == 512 and cap == 32:
            return fused(embeddings, cluster, rank)
        return local(embeddings, cluster, rank)

    return jax.shard_map(
        body,
        mesh=mesh,
        in_specs=(P(("parts", "blk"), None), P(("parts", "blk"), None), P(("parts", "blk"))),
        out_specs=P(("parts", "blk")),
        check_vma=False,
    )
```

```python
import functools

import jax
import jax.numpy as jnp
from jax import lax
from jax.experimental import pallas as pl
from jax.experimental.pallas import tpu as pltpu
from jax.sharding import PartitionSpec as P

MESH = pl.DeviceIdType.MESH
HIGHEST = lax.Precision.HIGHEST


def best_over(q_rows, q_rank, k_rows, k_rank):
    total = q_rows.shape[0]
    block_len = min(512, total)
    similar = lax.dot_general(
        q_rows, k_rows, (((1,), (1,)), ((), ())), preferred_element_type=jnp.float32
    )
    allowed = k_rank[None, :] > q_rank[0:block_len, None]
    pieces = jnp.max(jnp.where(allowed, similar, -1.0), axis=1)
    return pieces


def local(embeddings, cluster, rank):
    devices = lax.axis_size("blk")
    local_rows = embeddings.shape[0]
    width = embeddings.shape[1]
    slot_total = 2 * local_rows
    capacity = slot_total // devices
    floats = embeddings.astype(jnp.float32)
    unit_rows = (
        floats * lax.rsqrt(jnp.sum(floats * floats, axis=1, keepdims=True) + 1e-06)
    ).astype(jnp.bfloat16)
    target = cluster[:, 0]
    one_hot = (target[:, None] == jnp.arange(devices, dtype=jnp.int32)[None, :]).astype(jnp.int32)
    earlier = jnp.cumsum(one_hot, axis=0) - one_hot
    within = jnp.sum(earlier * one_hot, axis=1)
    slot_of = target * capacity + within
    send_rows = (
        jnp.zeros((slot_total, width), jnp.bfloat16)
        .at[slot_of]
        .set(unit_rows)
        .reshape(devices, capacity, width)
    )
    send_rank = (
        jnp.full((slot_total,), -1, jnp.int32).at[slot_of].set(rank).reshape(devices, capacity)
    )
    got_rows, got_rank = (
        lax.all_to_all(send_rows, "blk", split_axis=0, concat_axis=0, tiled=True),
        lax.all_to_all(send_rank, "blk", split_axis=0, concat_axis=0, tiled=True),
    )
    all_rows = got_rows.reshape(slot_total, width)
    all_rank = got_rank.reshape(slot_total)
    best_flat = best_over(all_rows, all_rank, all_rows, all_rank)
    returned = lax.all_to_all(
        best_flat.reshape(devices, capacity), "blk", split_axis=0, concat_axis=0, tiled=True
    )
    return returned.reshape(slot_total)[slot_of]


def kernel(
    n, cap, emb_hbm, cluster_hbm, rank_hbm, out_ref,
    emb, cluster_ref, rank_ref, send_rows, rows, send_rank, ranks, send_best, bests,
    load_sems, row_out, row_in, rank_out, rank_in, best_out, best_in, edge_in, half_in, all_in,
):
    me = lax.axis_index("blk")
    count, width = emb.shape
    slots = n * cap
    quarter = n // 4
    part = quarter * cap
    layer = me // quarter
    turn = me % quarter
    side = layer // 2
    early = quarter // 2
    middle = jnp.logical_or(layer == 1, layer == 2)
    near = 1 + layer % 2
    rim = 3 * side
    far_rim = 3 - rim
    last = 2 - side
    inward = near * quarter
    across = last * quarter
    own = me - turn

    barrier = pltpu.get_barrier_semaphore()
    loads = [
        pltpu.make_async_copy(source, into, load_sems.at[i])
        for i, (source, into) in enumerate(
            [(cluster_hbm, cluster_ref), (rank_hbm, rank_ref), (emb_hbm, emb)]
        )
    ]

    for load in loads:
        load.start()

    def signal(sem, to):
        pl.semaphore_signal(sem, inc=1, device_id={"blk": to}, device_id_type=MESH)

    @pl.when(middle)
    def _():
        @pl.loop(0, quarter)
        def _(k):
            signal(barrier, inward + k)

        @pl.loop(0, quarter)
        def _(k):
            signal(barrier, rim * quarter + k)

        @pl.loop(1, quarter)
        def _(k):
            signal(barrier, own + lax.rem(turn + k, quarter))

    @pl.when(jnp.logical_not(middle))
    def _():
        pl.semaphore_wait(barrier, quarter)

        @pl.loop(0, quarter)
        def _(k):
            signal(edge_in, inward + k)

    loads[0].wait()
    target = cluster_ref[...]
    ids = lax.broadcasted_iota(jnp.int32, (n, count), 0)
    named = (ids == target).astype(jnp.float32)
    before = lax.broadcasted_iota(jnp.int32, (count, count), 0)
    after = lax.broadcasted_iota(jnp.int32, (count, count), 1)
    upper = (before < after).astype(jnp.bfloat16)
    earlier = jnp.dot(named.astype(jnp.bfloat16), upper, preferred_element_type=jnp.float32)
    within = jnp.sum(earlier * named, axis=0, keepdims=True).astype(jnp.int32)
    slot_of = target * cap + within
    def choose(to):
        wanted = lax.broadcasted_iota(jnp.int32, (cap, count), 0) + to * cap
        return (wanted == slot_of).astype(jnp.bfloat16)

    def pack(to, pick=None):
        pick = choose(to) if pick is None else pick
        floats = jnp.dot(pick, emb[...], preferred_element_type=jnp.float32)
        scale = lax.rsqrt(jnp.sum(floats * floats, axis=1, keepdims=True) + 1e-06)
        send_rows[to] = (floats * scale).astype(jnp.bfloat16)

    def place_of(source, keeper):
        z = source // quarter
        end = 2 - keeper // (2 * quarter)
        step = source % quarter
        wait = lax.rem(step - keeper % quarter + 2 + quarter, quarter)
        return jnp.where(z == end, 3 * quarter + wait, (z + 1) // 2 * quarter + step)

    def row_copy(to, at=None):
        at = place_of(me, to) if at is None else at
        return pltpu.make_async_remote_copy(
            src_ref=send_rows.at[to], dst_ref=rows.at[at], send_sem=row_out.at[to],
            recv_sem=row_in.at[at], device_id={"blk": to}, device_id_type=MESH,
        )

    def rank_copy(to, at=None):
        at = place_of(me, to) if at is None else at
        return pltpu.make_async_remote_copy(
            src_ref=send_rank.at[to], dst_ref=ranks.at[at], send_sem=rank_out.at[to],
            recv_sem=rank_in.at[at], device_id={"blk": to}, device_id_type=MESH,
        )

    other = lax.rem(me + 1, n)
    home = place_of(me, me)

    per = 128 // cap

    def best_copy(to, at):
        return pltpu.make_async_remote_copy(
            src_ref=send_best.at[place_of(to, me) // per], dst_ref=bests.at[at], send_sem=best_out.at[to],
            recv_sem=best_in.at[at], device_id={"blk": to}, device_id_type=MESH,
        )

    def turned(k):
        odd = turn % 2
        cross = (1 - odd) * lax.rem(k + 1, 2) + odd * lax.rem((k + 1) // 2, 2)
        return lax.rem(turn // 2 + cross, 2) * 2 + lax.rem(turn + k // 2, 2)

    def pack_all(first, begin, end):
        @pl.loop(begin, end)
        def _(k):
            pack(first + turned(k))

    def send_all(first, begin, end):
        @pl.loop(begin, end)
        def _(k):
            row_copy(first + turned(k)).start()

    def pack_send(first, begin, end):
        @pl.loop(begin, end)
        def _(k):
            to = first + turned(k)
            pack(to)
            row_copy(to).start()

    lead = inward + turned(0)
    pick_lead = choose(lead)
    loads[2].wait()
    pack(lead, pick_lead)

    @pl.when(middle)
    def _():
        pl.semaphore_wait(barrier, 2 * quarter - 1)

    row_copy(lead).start()
    pack_send(inward, 1, 2)
    loads[1].wait()
    lanes = lax.broadcasted_iota(jnp.int32, (128, count), 0)
    spots = (lanes == within).astype(jnp.float32)
    placed = lax.dot_general(
        named * (rank_ref[...] + 1).astype(jnp.float32), spots, (((1,), (1,)), ((), ())),
        precision=HIGHEST, preferred_element_type=jnp.float32,
    )
    for c in range(n):
        send_rank[c] = placed[c:c + 1]

    def rank_all(first, begin):
        @pl.loop(begin, quarter)
        def _(k):
            rank_copy(first + lax.rem(turn + k, quarter)).start()

    def send_own():
        @pl.loop(1, quarter)
        def _(k):
            to = own + lax.rem(turn + k, quarter)
            pack(to)
            row_copy(to).start()

    rank_all(inward, 0)

    @pl.when(middle)
    def _():
        pl.semaphore_wait(edge_in, quarter)
        signal(half_in, inward + turn)
        rank_all(rim * quarter, 0)
        rank_all(own, 1)
        pack_send(inward, 2, early)
        pack_all(far_rim * quarter, 0, 2)
        pl.semaphore_wait(half_in, 1)
        signal(all_in, rim * quarter + turn)
        rank_all(far_rim * quarter, 0)
        send_all(far_rim * quarter, 0, 2)
        pack_send(far_rim * quarter, 2, quarter)
        pack_send(rim * quarter, 0, quarter)
        pack_send(inward, early, quarter)
        send_own()

    @pl.when(jnp.logical_not(middle))
    def _():
        pack_send(inward, 2, quarter)
        pack_all(far_rim * quarter, 0, quarter)
        pl.semaphore_wait(all_in, 1)
        rank_all(far_rim * quarter, 0)
        rank_all(across, 0)
        rank_all(own, 1)
        send_all(far_rim * quarter, 0, quarter)
        pack_send(across, 0, quarter)
        send_own()

    pack(me)
    rows[home] = send_rows[me]
    ranks[home] = send_rank[me]

    @pl.loop(1, n)
    def _(k):
        rank_copy(lax.rem(me + k, n)).wait_send()

    @pl.loop(0, n)
    def _(k):
        @pl.when(k != home)
        def _():
            rank_copy(other, k).wait_recv()

    held = jnp.concatenate([ranks[c] for c in range(n)], axis=0)
    source = lax.broadcasted_iota(jnp.int32, (n, slots), 0)
    slot = lax.broadcasted_iota(jnp.int32, (n, slots), 1)
    spread = (slot // cap == source).astype(jnp.float32)
    wide = lax.dot_general(
        held, spread, (((0,), (0,)), ((), ())),
        precision=HIGHEST, preferred_element_type=jnp.float32,
    )
    lane_of = lax.broadcasted_iota(jnp.int32, (128, slots), 0)
    slot_in = lax.broadcasted_iota(jnp.int32, (128, slots), 1) % cap
    rank_row = jnp.sum(jnp.where(lane_of == slot_in, wide, 0.0), axis=0, keepdims=True)
    down = lax.dot_general(
        spread, held, (((0,), (0,)), ((), ())),
        precision=HIGHEST, preferred_element_type=jnp.float32,
    )
    lane_at = lax.broadcasted_iota(jnp.int32, (slots, 128), 1)
    slot_at = lax.broadcasted_iota(jnp.int32, (slots, 128), 0) % cap
    rank_col = jnp.sum(jnp.where(lane_at == slot_at, down, 0.0), axis=1, keepdims=True)

    def best_of(keys, key_rank, queries, query_rank):
        similar = lax.dot_general(
            keys, queries, (((1,), (1,)), ((), ())), preferred_element_type=jnp.float32
        )
        return jnp.max(jnp.where(key_rank > query_rank, similar, -1.0), axis=0, keepdims=True)

    def arrive(begin, end):
        @pl.loop(begin, end)
        def _(k):
            @pl.when(k != home)
            def _():
                row_copy(other, k).wait_recv()

    def send_back(begin, end):
        @pl.loop(begin, end)
        def _(to):
            @pl.when(to != me)
            def _():
                best_copy(to, me).start()

    def span(begin, end):
        return rows[begin:end].reshape((end - begin) * cap, width)

    early_row, late_row = rank_row[:, :3 * part], rank_row[:, 3 * part:]
    early_col, late_col = rank_col[:3 * part], rank_col[3 * part:]
    arrive(0, n - quarter)
    best_early = best_of(span(0, n - quarter), early_col, span(0, n - quarter), early_row)
    arrive(n - quarter, n)
    fresh = span(n - quarter, n)
    send_best[0] = jnp.maximum(
        best_early[:, :part], best_of(fresh, late_col, span(0, quarter), early_row[:, :part])
    )
    send_back(0, quarter)
    best_rest = jnp.maximum(
        best_early[:, part:],
        best_of(fresh, late_col, span(quarter, n - quarter), early_row[:, part:]),
    )
    best_late = jnp.maximum(
        best_of(span(0, n - quarter), early_col, fresh, late_row),
        best_of(fresh, late_col, fresh, late_row),
    )
    send_best[1] = best_rest[:, :part]
    send_best[2] = best_rest[:, part:]
    send_best[3] = best_late
    send_back(quarter, n)
    bests[me] = send_best[home // per]

    keeper = lax.broadcasted_iota(jnp.int32, (n, 128), 0)
    offset = jnp.zeros((n, 128), jnp.int32)
    for c in range(n):
        offset = jnp.where(keeper == c, place_of(me, c) % per * cap, offset)

    @pl.loop(0, n)
    def _(to):
        @pl.when(to != me)
        def _():
            row_copy(to).wait_send()

    @pl.loop(1, n)
    def _(k):
        at = lax.rem(me + k, n)
        best_copy(at, at).wait()

    mine = jnp.concatenate([bests[c] for c in range(n)], axis=0)
    for k in range(count // 128):
        piece = slice(128 * k, 128 * (k + 1))
        at = offset + within[:, piece]
        found = jnp.take_along_axis(mine, at, axis=1, mode="promise_in_bounds")
        out_ref[:, piece] = jnp.sum(
            jnp.where(named[:, piece] > 0.0, found, 0.0), axis=0, keepdims=True
        )


def fused(embeddings, cluster, rank):
    n = lax.axis_size("blk")
    count, width = embeddings.shape
    cap = 2 * count // n
    slots = n * cap
    vmem = pl.BlockSpec(memory_space=pltpu.VMEM)
    best = pl.pallas_call(
        functools.partial(kernel, n, cap),
        out_shape=pltpu.VMEM((1, count), jnp.float32),
        in_specs=[pl.BlockSpec(memory_space=pl.ANY)] * 3,
        out_specs=vmem,
        scratch_shapes=[
            pltpu.VMEM((count, width), jnp.bfloat16),
            pltpu.VMEM((1, count), jnp.int32),
            pltpu.VMEM((1, count), jnp.int32),
            pltpu.VMEM((n, cap, width), jnp.bfloat16),
            pltpu.VMEM((n, cap, width), jnp.bfloat16),
            pltpu.VMEM((n, 1, 128), jnp.float32),
            pltpu.VMEM((n, 1, 128), jnp.float32),
            pltpu.VMEM((slots // 128, 1, 128), jnp.float32),
            pltpu.VMEM((n, 1, 128), jnp.float32),
            pltpu.SemaphoreType.DMA((3,)),
        ] + [pltpu.SemaphoreType.DMA((n,))] * 6 + [pltpu.SemaphoreType.REGULAR] * 3,
        compiler_params=pltpu.CompilerParams(collective_id=0, has_side_effects=True),
    )(embeddings, cluster.reshape(1, count), rank.reshape(1, count))
    return best.reshape(count)


def solution(mesh):
    def body(embeddings, cluster, rank):
        n = lax.axis_size("blk")
        slots = 2 * embeddings.shape[0]
        cap = slots // n
        if n == 16 and slots == 512 and cap == 32:
            return fused(embeddings, cluster, rank)
        return local(embeddings, cluster, rank)

    return jax.shard_map(
        body,
        mesh=mesh,
        in_specs=(P(("parts", "blk"), None), P(("parts", "blk"), None), P(("parts", "blk"))),
        out_specs=P(("parts", "blk")),
        check_vma=False,
    )
```

```python
import functools

import jax
import jax.numpy as jnp
from jax import lax
from jax.experimental import pallas as pl
from jax.experimental.pallas import tpu as pltpu
from jax.sharding import PartitionSpec as P

MESH = pl.DeviceIdType.MESH
HIGHEST = lax.Precision.HIGHEST


def best_over(q_rows, q_rank, k_rows, k_rank):
    total = q_rows.shape[0]
    block_len = min(512, total)
    similar = lax.dot_general(
        q_rows, k_rows, (((1,), (1,)), ((), ())), preferred_element_type=jnp.float32
    )
    allowed = k_rank[None, :] > q_rank[0:block_len, None]
    pieces = jnp.max(jnp.where(allowed, similar, -1.0), axis=1)
    return pieces


def local(embeddings, cluster, rank):
    devices = lax.axis_size("blk")
    local_rows = embeddings.shape[0]
    width = embeddings.shape[1]
    slot_total = 2 * local_rows
    capacity = slot_total // devices
    floats = embeddings.astype(jnp.float32)
    unit_rows = (
        floats * lax.rsqrt(jnp.sum(floats * floats, axis=1, keepdims=True) + 1e-06)
    ).astype(jnp.bfloat16)
    target = cluster[:, 0]
    one_hot = (target[:, None] == jnp.arange(devices, dtype=jnp.int32)[None, :]).astype(jnp.int32)
    earlier = jnp.cumsum(one_hot, axis=0) - one_hot
    within = jnp.sum(earlier * one_hot, axis=1)
    slot_of = target * capacity + within
    send_rows = (
        jnp.zeros((slot_total, width), jnp.bfloat16)
        .at[slot_of]
        .set(unit_rows)
        .reshape(devices, capacity, width)
    )
    send_rank = (
        jnp.full((slot_total,), -1, jnp.int32).at[slot_of].set(rank).reshape(devices, capacity)
    )
    got_rows, got_rank = (
        lax.all_to_all(send_rows, "blk", split_axis=0, concat_axis=0, tiled=True),
        lax.all_to_all(send_rank, "blk", split_axis=0, concat_axis=0, tiled=True),
    )
    all_rows = got_rows.reshape(slot_total, width)
    all_rank = got_rank.reshape(slot_total)
    best_flat = best_over(all_rows, all_rank, all_rows, all_rank)
    returned = lax.all_to_all(
        best_flat.reshape(devices, capacity), "blk", split_axis=0, concat_axis=0, tiled=True
    )
    return returned.reshape(slot_total)[slot_of]


def kernel(
    n, cap, emb_hbm, cluster_hbm, rank_hbm, out_ref,
    emb, cluster_ref, rank_ref, send_rows, rows, send_rank, ranks, send_best, bests,
    load_sems, row_out, row_in, rank_out, rank_in, best_out, best_in, edge_in, half_in, all_in,
):
    me = lax.axis_index("blk")
    count, width = emb.shape
    slots = n * cap
    quarter = n // 4
    part = quarter * cap
    layer = me // quarter
    turn = me % quarter
    side = layer // 2
    early = quarter // 2
    middle = jnp.logical_or(layer == 1, layer == 2)
    near = 1 + layer % 2
    rim = 3 * side
    far_rim = 3 - rim
    last = 2 - side
    inward = near * quarter
    across = last * quarter
    own = me - turn

    barrier = pltpu.get_barrier_semaphore()
    loads = [
        pltpu.make_async_copy(source, into, load_sems.at[i])
        for i, (source, into) in enumerate(
            [(cluster_hbm, cluster_ref), (rank_hbm, rank_ref), (emb_hbm, emb)]
        )
    ]

    for load in loads:
        load.start()

    def signal(sem, to):
        pl.semaphore_signal(sem, inc=1, device_id={"blk": to}, device_id_type=MESH)

    @pl.when(middle)
    def _():
        @pl.loop(0, quarter)
        def _(k):
            signal(barrier, inward + k)

        @pl.loop(0, quarter)
        def _(k):
            signal(barrier, rim * quarter + k)

        @pl.loop(1, quarter)
        def _(k):
            signal(barrier, own + lax.rem(turn + k, quarter))

    @pl.when(jnp.logical_not(middle))
    def _():
        pl.semaphore_wait(barrier, quarter)

        @pl.loop(0, quarter)
        def _(k):
            signal(edge_in, inward + k)

    loads[0].wait()
    target = cluster_ref[...]
    ids = lax.broadcasted_iota(jnp.int32, (n, count), 0)
    named = (ids == target).astype(jnp.float32)
    before = lax.broadcasted_iota(jnp.int32, (count, count), 0)
    after = lax.broadcasted_iota(jnp.int32, (count, count), 1)
    upper = (before < after).astype(jnp.bfloat16)
    earlier = jnp.dot(named.astype(jnp.bfloat16), upper, preferred_element_type=jnp.float32)
    within = jnp.sum(earlier * named, axis=0, keepdims=True).astype(jnp.int32)
    slot_of = target * cap + within
    def choose(to):
        wanted = lax.broadcasted_iota(jnp.int32, (cap, count), 0) + to * cap
        return (wanted == slot_of).astype(jnp.bfloat16)

    def pack(to, pick=None):
        pick = choose(to) if pick is None else pick
        floats = jnp.dot(pick, emb[...], preferred_element_type=jnp.float32)
        scale = lax.rsqrt(jnp.sum(floats * floats, axis=1, keepdims=True) + 1e-06)
        send_rows[to] = (floats * scale).astype(jnp.bfloat16)

    def place_of(source, keeper):
        z = source // quarter
        end = 2 - keeper // (2 * quarter)
        step = source % quarter
        wait = lax.rem(step - keeper % quarter + 2 + quarter, quarter)
        return jnp.where(z == end, 3 * quarter + wait, (z + 1) // 2 * quarter + step)

    def row_copy(to, at=None):
        at = place_of(me, to) if at is None else at
        return pltpu.make_async_remote_copy(
            src_ref=send_rows.at[to], dst_ref=rows.at[at], send_sem=row_out.at[to],
            recv_sem=row_in.at[at], device_id={"blk": to}, device_id_type=MESH,
        )

    def rank_copy(to, at=None):
        at = place_of(me, to) if at is None else at
        return pltpu.make_async_remote_copy(
            src_ref=send_rank.at[to], dst_ref=ranks.at[at], send_sem=rank_out.at[to],
            recv_sem=rank_in.at[at], device_id={"blk": to}, device_id_type=MESH,
        )

    other = lax.rem(me + 1, n)
    home = place_of(me, me)

    per = 128 // cap

    def best_copy(to, at):
        return pltpu.make_async_remote_copy(
            src_ref=send_best.at[place_of(to, me) // per], dst_ref=bests.at[at], send_sem=best_out.at[to],
            recv_sem=best_in.at[at], device_id={"blk": to}, device_id_type=MESH,
        )

    def turned(k):
        odd = turn % 2
        cross = (1 - odd) * lax.rem(k + 1, 2) + odd * lax.rem((k + 1) // 2, 2)
        return lax.rem(turn // 2 + cross, 2) * 2 + lax.rem(turn + k // 2, 2)

    def pack_all(first, begin, end):
        for k in range(begin, end):
            pack(first + turned(k))

    def send_all(first, begin, end):
        @pl.loop(begin, end)
        def _(k):
            row_copy(first + turned(k)).start()

    def pack_send(first, begin, end):
        for k in range(begin, end):
            to = first + turned(k)
            pack(to)
            row_copy(to).start()

    lead = inward + turned(0)
    pick_lead = choose(lead)
    loads[2].wait()
    pack(lead, pick_lead)

    @pl.when(middle)
    def _():
        pl.semaphore_wait(barrier, 2 * quarter - 1)

    row_copy(lead).start()
    pack_send(inward, 1, 2)
    loads[1].wait()
    lanes = lax.broadcasted_iota(jnp.int32, (128, count), 0)
    spots = (lanes == within).astype(jnp.float32)
    placed = lax.dot_general(
        named * (rank_ref[...] + 1).astype(jnp.float32), spots, (((1,), (1,)), ((), ())),
        precision=HIGHEST, preferred_element_type=jnp.float32,
    )
    for c in range(n):
        send_rank[c] = placed[c:c + 1]

    def rank_all(first, begin):
        @pl.loop(begin, quarter)
        def _(k):
            rank_copy(first + lax.rem(turn + k, quarter)).start()

    def send_own():
        for k in range(1, quarter):
            to = own + lax.rem(turn + k, quarter)
            pack(to)
            row_copy(to).start()

    rank_all(inward, 0)

    @pl.when(middle)
    def _():
        pl.semaphore_wait(edge_in, quarter)
        signal(half_in, inward + turn)
        rank_all(rim * quarter, 0)
        rank_all(own, 1)
        pack_send(inward, 2, early)
        pack_all(far_rim * quarter, 0, 2)
        pl.semaphore_wait(half_in, 1)
        signal(all_in, rim * quarter + turn)
        rank_all(far_rim * quarter, 0)
        send_all(far_rim * quarter, 0, 2)
        pack_send(far_rim * quarter, 2, quarter)
        pack_send(rim * quarter, 0, quarter)
        pack_send(inward, early, quarter)
        send_own()

    @pl.when(jnp.logical_not(middle))
    def _():
        pack_send(inward, 2, quarter)
        pack_all(far_rim * quarter, 0, quarter)
        pl.semaphore_wait(all_in, 1)
        rank_all(far_rim * quarter, 0)
        rank_all(across, 0)
        rank_all(own, 1)
        send_all(far_rim * quarter, 0, quarter)
        pack_send(across, 0, quarter)
        send_own()

    pack(me)
    rows[home] = send_rows[me]
    ranks[home] = send_rank[me]

    @pl.loop(1, n)
    def _(k):
        rank_copy(lax.rem(me + k, n)).wait_send()

    @pl.loop(0, n)
    def _(k):
        @pl.when(k != home)
        def _():
            rank_copy(other, k).wait_recv()

    held = jnp.concatenate([ranks[c] for c in range(n)], axis=0)
    source = lax.broadcasted_iota(jnp.int32, (n, slots), 0)
    slot = lax.broadcasted_iota(jnp.int32, (n, slots), 1)
    spread = (slot // cap == source).astype(jnp.float32)
    wide = lax.dot_general(
        held, spread, (((0,), (0,)), ((), ())),
        precision=HIGHEST, preferred_element_type=jnp.float32,
    )
    lane_of = lax.broadcasted_iota(jnp.int32, (128, slots), 0)
    slot_in = lax.broadcasted_iota(jnp.int32, (128, slots), 1) % cap
    rank_row = jnp.sum(jnp.where(lane_of == slot_in, wide, 0.0), axis=0, keepdims=True)
    down = lax.dot_general(
        spread, held, (((0,), (0,)), ((), ())),
        precision=HIGHEST, preferred_element_type=jnp.float32,
    )
    lane_at = lax.broadcasted_iota(jnp.int32, (slots, 128), 1)
    slot_at = lax.broadcasted_iota(jnp.int32, (slots, 128), 0) % cap
    rank_col = jnp.sum(jnp.where(lane_at == slot_at, down, 0.0), axis=1, keepdims=True)

    def best_of(keys, key_rank, queries, query_rank):
        similar = lax.dot_general(
            keys, queries, (((1,), (1,)), ((), ())), preferred_element_type=jnp.float32
        )
        return jnp.max(jnp.where(key_rank > query_rank, similar, -1.0), axis=0, keepdims=True)

    def arrive(begin, end):
        @pl.loop(begin, end)
        def _(k):
            @pl.when(k != home)
            def _():
                row_copy(other, k).wait_recv()

    def send_back(begin, end):
        for to in range(begin, end):
            @pl.when(to != me)
            def _():
                best_copy(to, me).start()

    def span(begin, end):
        return rows[begin:end].reshape((end - begin) * cap, width)

    early_row, late_row = rank_row[:, :3 * part], rank_row[:, 3 * part:]
    early_col, late_col = rank_col[:3 * part], rank_col[3 * part:]
    arrive(0, n - quarter)
    best_early = best_of(span(0, n - quarter), early_col, span(0, n - quarter), early_row)
    arrive(n - quarter, n)
    fresh = span(n - quarter, n)
    send_best[0] = jnp.maximum(
        best_early[:, :part], best_of(fresh, late_col, span(0, quarter), early_row[:, :part])
    )
    send_back(0, quarter)
    best_rest = jnp.maximum(
        best_early[:, part:],
        best_of(fresh, late_col, span(quarter, n - quarter), early_row[:, part:]),
    )
    best_late = jnp.maximum(
        best_of(span(0, n - quarter), early_col, fresh, late_row),
        best_of(fresh, late_col, fresh, late_row),
    )
    send_best[1] = best_rest[:, :part]
    send_best[2] = best_rest[:, part:]
    send_best[3] = best_late
    send_back(quarter, n)
    bests[me] = send_best[home // per]

    keeper = lax.broadcasted_iota(jnp.int32, (n, 128), 0)
    offset = jnp.zeros((n, 128), jnp.int32)
    for c in range(n):
        offset = jnp.where(keeper == c, place_of(me, c) % per * cap, offset)

    @pl.loop(0, n)
    def _(to):
        @pl.when(to != me)
        def _():
            row_copy(to).wait_send()

    def best_arrive(begin, end):
        @pl.loop(begin, end)
        def _(at):
            @pl.when(at != me)
            def _():
                best_copy(at, at).wait_recv()

    best_arrive(0, quarter)
    best_arrive(3 * quarter, n)

    @pl.loop(1, n)
    def _(k):
        at = lax.rem(me + k, n)
        best_copy(at, at).wait_send()

    best_arrive(quarter, 3 * quarter)

    mine = jnp.concatenate([bests[c] for c in range(n)], axis=0)
    for k in range(count // 128):
        piece = slice(128 * k, 128 * (k + 1))
        at = offset + within[:, piece]
        found = jnp.take_along_axis(mine, at, axis=1, mode="promise_in_bounds")
        out_ref[:, piece] = jnp.sum(
            jnp.where(named[:, piece] > 0.0, found, 0.0), axis=0, keepdims=True
        )


def fused(embeddings, cluster, rank):
    n = lax.axis_size("blk")
    count, width = embeddings.shape
    cap = 2 * count // n
    slots = n * cap
    vmem = pl.BlockSpec(memory_space=pltpu.VMEM)
    best = pl.pallas_call(
        functools.partial(kernel, n, cap),
        out_shape=pltpu.VMEM((1, count), jnp.float32),
        in_specs=[pl.BlockSpec(memory_space=pl.ANY)] * 3,
        out_specs=vmem,
        scratch_shapes=[
            pltpu.VMEM((count, width), jnp.bfloat16),
            pltpu.VMEM((1, count), jnp.int32),
            pltpu.VMEM((1, count), jnp.int32),
            pltpu.VMEM((n, cap, width), jnp.bfloat16),
            pltpu.VMEM((n, cap, width), jnp.bfloat16),
            pltpu.VMEM((n, 1, 128), jnp.float32),
            pltpu.VMEM((n, 1, 128), jnp.float32),
            pltpu.VMEM((slots // 128, 1, 128), jnp.float32),
            pltpu.VMEM((n, 1, 128), jnp.float32),
            pltpu.SemaphoreType.DMA((3,)),
        ] + [pltpu.SemaphoreType.DMA((n,))] * 6 + [pltpu.SemaphoreType.REGULAR] * 3,
        compiler_params=pltpu.CompilerParams(collective_id=0, has_side_effects=True),
    )(embeddings, cluster.reshape(1, count), rank.reshape(1, count))
    return best.reshape(count)


def solution(mesh):
    def body(embeddings, cluster, rank):
        n = lax.axis_size("blk")
        slots = 2 * embeddings.shape[0]
        cap = slots // n
        if n == 16 and slots == 512 and cap == 32:
            return fused(embeddings, cluster, rank)
        return local(embeddings, cluster, rank)

    return jax.shard_map(
        body,
        mesh=mesh,
        in_specs=(P(("parts", "blk"), None), P(("parts", "blk"), None), P(("parts", "blk"))),
        out_specs=P(("parts", "blk")),
        check_vma=False,
    )
```
